32 devices in a mesh: freq: 4 (over y, x), space: 8 (over z, core).
Axes of the slice: x: 2, y: 2, z: 4, core: 2. Of those that a mesh axis runs over, the one named last changes fastest.
Arguments:
- snapshots: float32 [2, 256, 3, 4096], P(None, 'freq', None, 'space'), may hold values from -6 to 6
- mean_field: float32 [3, 4096], P(None, 'space'), may hold values from -3 to 3
- weights: float32 [3, 4096], P(None, 'space'), may hold values from 0.25 to 4
- rates: float32 [128], P('freq'), may hold values from 0.2 to 0.8
- modes: float32 [128, 2, 16, 3, 4096], P('freq', None, None, None, 'space'), may hold values from -6 to 6
Outputs:
- modes_out: float32 [128, 2, 16, 3, 4096], P('freq', None, None, None, 'space')
- coefficients: float32 [2, 128, 2, 16], P(None, 'freq')
The draws below stay inside these ranges and needn't reach their ends.
All inputs are finite; a program needn't handle non-finite values.
Results may differ from the reference program's by a relative error of at most 0.00024.
Values sent between devices are 32-bit elements; how exact they have to be, the bound alone decides.
A program may use at most 64 MiB of HBM per device.

```python
import math
import jax
import jax.numpy as jnp
from jax import lax

NT = 256
NF = 128
K = 16
FIELDS = 3
BLOCKS = 2
POINTS = 4096


def steps_of(rng, shape, cuts, least, largest):
    level = 1.0
    for dim, blocks in cuts:
        heights = jax.random.uniform(jax.random.fold_in(jax.random.fold_in(rng, 6), dim), (blocks,), jnp.float32, least / len(cuts), largest / len(cuts))
        level = level * jnp.repeat(jnp.exp(heights), shape[dim] // blocks).reshape((-1,) + (1,) * (len(shape) - 1 - dim))
    return level


def scatter_about(key, dims, width, reach, split=(), held_as=jnp.bfloat16):
    values = width * jax.random.normal(key, dims, jnp.float32)
    if split:
        values = values * steps_of(key, dims, split, -0.22, 0.18)
    return jnp.clip(values, -reach, reach).astype(held_as)


def setup_inputs(seed: int = 0) -> dict:
    splits = jax.random.split(jax.random.key(seed), 6)
    snapshots = scatter_about(splits[0], (BLOCKS, NT, FIELDS, POINTS), 1.0, 6.0, ((1, 4), (3, 8)), jnp.float32)
    mean_field = scatter_about(splits[1], (FIELDS, POINTS), 0.5, 3.0, ((1, 8),), jnp.float32)
    weights = jnp.clip(jnp.exp(math.log(4.0) - 2.7725887 * jax.random.uniform(splits[2], (FIELDS, POINTS), jnp.float32) ** steps_of(splits[2], (FIELDS, POINTS), ((1, 8),), -0.2, 0.2)), 0.25, 4.0)
    rates = jnp.clip(jnp.exp(math.log(0.8) - 1.3862944 * jax.random.uniform(splits[3], (NF,), jnp.float32) ** steps_of(splits[3], (NF,), ((0, 4),), -0.2, 0.2)), 0.2, 0.8)
    modes = scatter_about(splits[4], (NF, 2, K, FIELDS, POINTS), 1.0, 6.0, ((0, 4), (4, 8)), jnp.float32)
    return dict(snapshots=snapshots, mean_field=mean_field, weights=weights, rates=rates, modes=modes)


def project(matrix, vector):
    return jnp.einsum('fkcp,fcp->fk', matrix, vector, precision=lax.Precision.HIGHEST)

def combine(coefs, matrix):
    return jnp.einsum('fk,fkcp->fcp', coefs, matrix, precision=lax.Precision.HIGHEST)

def reference(snapshots, mean_field, weights, rates, modes):
    times = jnp.arange(NT, dtype=jnp.float32)
    window = 0.5 - 0.5 * jnp.cos(2.0 * math.pi / NT * times)
    scale_factor = 1.0 / math.sqrt(3.0 * NT / 8.0)
    point_count = FIELDS * POINTS
    root_count = math.sqrt(point_count)
    modes_real = modes[:, 0]
    modes_imag = modes[:, 1]
    coef_list = []
    for block in range(BLOCKS):
        centered = (snapshots[block] - mean_field[None]) * window[:, None, None]
        spectra = jnp.fft.rfft(centered, axis=0)[:NF] * scale_factor
        spec_real = jnp.real(spectra).astype(jnp.float32)
        spec_imag = jnp.imag(spectra).astype(jnp.float32)
        weighted_real = weights[None] * spec_real
        weighted_imag = weights[None] * spec_imag
        coefs_real = (project(modes_real, weighted_real) + project(modes_imag, weighted_imag)) / root_count
        coefs_imag = (project(modes_real, weighted_imag) - project(modes_imag, weighted_real)) / root_count
        energy = lax.optimization_barrier(jnp.sum(weighted_real * spec_real + weighted_imag * spec_imag, axis=(1, 2))) / point_count
        coef_list.append(jnp.stack((coefs_real, coefs_imag), axis=1))
        resid_real = spec_real - (combine(coefs_real, modes_real) - combine(coefs_imag, modes_imag)) / root_count
        resid_imag = spec_imag - (combine(coefs_real, modes_imag) + combine(coefs_imag, modes_real)) / root_count
        gain = rates / jnp.sqrt(energy + 1e-06)
        steps_real = (gain[:, None] * coefs_real)[:, :, None, None]
        steps_imag = (-gain[:, None] * coefs_imag)[:, :, None, None]
        fresh_real = modes_real + steps_real * resid_real[:, None] - steps_imag * resid_imag[:, None]
        fresh_imag = modes_imag + steps_real * resid_imag[:, None] + steps_imag * resid_real[:, None]
        norms = lax.optimization_barrier(jnp.sum(weights[None, None] * (fresh_real * fresh_real + fresh_imag * fresh_imag), axis=(2, 3))) / point_count
        divisor = jnp.sqrt(norms + 1e-06)[:, :, None, None]
        modes_real = fresh_real / divisor
        modes_imag = fresh_imag / divisor
    return (jnp.stack((modes_real, modes_imag), axis=1), jnp.stack(coef_list, axis=0))
```

```python
import functools
import math

import jax
import jax.numpy as jnp
import numpy as np
from jax import lax
from jax.experimental import pallas as pl
from jax.experimental.pallas import tpu as pltpu
from jax.sharding import PartitionSpec as P

HIGHEST = lax.Precision.HIGHEST
LANES = 128


def spectral_table(length, parts):
    freqs = np.arange(length // 2)
    times = np.arange(length)
    angle = 2.0 * np.pi / length * (freqs[:, None] * times[None, :] % length)
    row = (0.5 - 0.5 * np.cos(2.0 * np.pi / length * times)) / math.sqrt(3.0 * length / 8.0)
    table = np.stack((np.cos(angle) * row, -np.sin(angle) * row))
    table = table.reshape(2, parts, -1, length).transpose(1, 0, 2, 3)
    return table.reshape(length, length).astype(np.float32)


def fold(value):
    total = value[:, :LANES]
    for start in range(LANES, value.shape[1], LANES):
        total = total + value[:, start : start + LANES]
    return total


def mul(x, y):
    return x[0] * y[0] - x[1] * y[1], x[0] * y[1] + x[1] * y[0]


def sub(x, y):
    return x[0] - y[0], x[1] - y[1]


def add(x, y):
    return x[0] + y[0], x[1] + y[1]


def conj(x):
    return x[0], -x[1]


def scale(s, x):
    return s * x[0], s * x[1]


def total(x):
    return jnp.sum(x[0], axis=0, keepdims=True), jnp.sum(x[1], axis=0, keepdims=True)


def spectra_kernel(
    nq, ns, point_count,
    snap, mean, weights, rates, table, modes_hbm,
    spec, coef, co,
    phi, recv, whole, wq, gs, gbuf, pbuf,
    phi_sem, own1_sem, own2_sem, send1, recv1, send2, recv2, send_g, recv_g, send_p, recv_p,
):
    blocks, fields, quarter, points = snap.shape
    freqs, _, _, modes_k, _ = phi.shape
    sub_points = points // nq
    groups = phi_sem.shape[0]
    per = freqs // groups
    me_q = lax.axis_index("freq")
    me_s = lax.axis_index("space")

    for g in range(groups):
        pltpu.make_async_copy(
            modes_hbm.at[pl.ds(g * per, per)], phi.at[pl.ds(g * per, per)], phi_sem.at[g]
        ).start()

    barrier = pltpu.get_barrier_semaphore()
    for d in range(1, nq):
        pl.semaphore_signal(
            barrier, inc=1, device_id={"freq": lax.rem(me_q + d, nq)},
            device_id_type=pl.DeviceIdType.MESH,
        )
    for d in range(1, ns):
        pl.semaphore_signal(
            barrier, inc=1, device_id={"space": lax.rem(me_s + d, ns)},
            device_id_type=pl.DeviceIdType.MESH,
        )
    pl.semaphore_wait(barrier, nq + ns - 2)

    def lanes_of(q):
        return pl.ds(pl.multiple_of(q * sub_points, LANES), sub_points)

    def times_of(q):
        return pl.ds(pl.multiple_of(q * quarter, 8), quarter)

    def copy1(b, d):
        to = lax.rem(me_q + d, nq)
        return pltpu.make_async_remote_copy(
            src_ref=snap.at[b, :, :, lanes_of(to)],
            dst_ref=recv.at[b, :, times_of(me_q), :],
            send_sem=send1.at[b, d], recv_sem=recv1.at[b, d],
            device_id={"freq": to}, device_id_type=pl.DeviceIdType.MESH,
        )

    def own1(b):
        return pltpu.make_async_copy(
            snap.at[b, :, :, lanes_of(me_q)], recv.at[b, :, times_of(me_q), :], own1_sem.at[b]
        )

    def copy2(b, d):
        to = lax.rem(me_q + d, nq)
        return pltpu.make_async_remote_copy(
            src_ref=whole.at[b, to],
            dst_ref=spec.at[b, :, :, lanes_of(me_q)],
            send_sem=send2.at[b, d], recv_sem=recv2.at[b, d],
            device_id={"freq": to}, device_id_type=pl.DeviceIdType.MESH,
        )

    def own2(b):
        return pltpu.make_async_copy(
            whole.at[b, me_q], spec.at[b, :, :, lanes_of(me_q)], own2_sem.at[b]
        )

    def copy_g(d):
        return pltpu.make_async_remote_copy(
            src_ref=gbuf.at[me_s], dst_ref=gbuf.at[me_s],
            send_sem=send_g.at[d], recv_sem=recv_g.at[d],
            device_id={"space": lax.rem(me_s + d, ns)}, device_id_type=pl.DeviceIdType.MESH,
        )

    def copy_p(b, d):
        return pltpu.make_async_remote_copy(
            src_ref=pbuf.at[b, me_s], dst_ref=pbuf.at[b, me_s],
            send_sem=send_p.at[b, d], recv_sem=recv_p.at[b, d],
            device_id={"space": lax.rem(me_s + d, ns)}, device_id_type=pl.DeviceIdType.MESH,
        )

    for b in range(blocks):
        for d in range(1, nq):
            copy1(b, d).start()
        own1(b).start()

    def gram(g):
        pltpu.make_async_copy(
            modes_hbm.at[pl.ds(g * per, per)], phi.at[pl.ds(g * per, per)], phi_sem.at[g]
        ).wait()
        rows = per * 2 * modes_k
        product = jnp.zeros((rows, rows), jnp.float32)
        for c in range(fields):
            left = phi[pl.ds(g * per, per), :, c].reshape(rows, points)
            product = product + lax.dot_general(
                left, left * weights[c : c + 1, :], (((1,), (1,)), ((), ())),
                precision=HIGHEST, preferred_element_type=jnp.float32,
            )
        lane = lax.broadcasted_iota(jnp.int32, (modes_k, LANES), 1)
        for f in range(per):
            start = f * 2 * modes_k
            tile = start // LANES * LANES
            block = product[start : start + 2 * modes_k, tile : tile + LANES]
            if start % LANES:
                block = pltpu.roll(block, LANES - start % LANES, 1)
            moved = pltpu.roll(block, LANES - modes_k, 1)
            real = block[:modes_k] + moved[modes_k:]
            imag = moved[:modes_k] - block[modes_k:]
            joined = jnp.where(lane < modes_k, real, pltpu.roll(imag, modes_k, 1))
            gs[pl.ds((g * per + f) * modes_k, modes_k), :] = joined

    def dft(b):
        own1(b).wait()
        for d in range(1, nq):
            copy1(b, d).wait_recv()
        for c in range(fields):
            centered = recv[b, c] - mean[c : c + 1, lanes_of(me_q)]
            rows = jnp.dot(
                table[...], centered, precision=HIGHEST, preferred_element_type=jnp.float32
            )
            whole[b, :, c] = rows.reshape(nq, 2 * freqs, sub_points)
        for d in range(1, nq):
            copy2(b, d).start()
        own2(b).start()

    def inner(b):
        own2(b).wait()
        for d in range(1, nq):
            copy2(b, d).wait_recv()
        energy = cross_r = cross_i = jnp.zeros((freqs, LANES), jnp.float32)
        for c in range(fields):
            plain = spec[b, c]
            heavy = plain * weights[c : c + 1, :]
            wq[c] = heavy
            real, imag = heavy[:freqs], heavy[freqs:]
            energy = energy + fold(real * plain[:freqs] + imag * plain[freqs:])
            if b:
                old_r, old_i = spec[b - 1, c, :freqs], spec[b - 1, c, freqs:]
                cross_r = cross_r + fold(old_r * real + old_i * imag)
                cross_i = cross_i + fold(old_r * imag - old_i * real)
        stacked = jnp.concatenate(
            [energy, cross_r, cross_i, jnp.zeros((LANES - 3 * freqs, LANES), jnp.float32)], axis=0
        )
        extra = jnp.sum(stacked.T, axis=0, keepdims=True)
        lane = lax.broadcasted_iota(jnp.int32, (modes_k, LANES), 1)

        def body(f, result):
            sum_r = jnp.zeros((modes_k, points), jnp.float32)
            sum_i = sum_r
            for c in range(fields):
                pr, pi = phi[f, 0, c], phi[f, 1, c]
                qr, qi = wq[c, pl.ds(f, 1), :], wq[c, pl.ds(freqs + f, 1), :]
                sum_r = sum_r + pr * qr + pi * qi
                sum_i = sum_i + pr * qi - pi * qr
            one_r = jnp.sum(fold(sum_r), axis=1, keepdims=True)
            one_i = jnp.sum(fold(sum_i), axis=1, keepdims=True)
            result = jnp.where(lane == f, one_r, result)
            return jnp.where(lane == freqs + f, one_i, result)

        result = lax.fori_loop(
            0, freqs, body, jnp.zeros((modes_k, LANES), jnp.float32), unroll=4
        )
        pbuf[b, me_s, pl.ds(0, modes_k), :] = result
        pbuf[b, me_s, pl.ds(modes_k, 8), :] = jnp.broadcast_to(extra, (8, LANES))
        for d in range(1, ns):
            copy_p(b, d).start()

    lax.fori_loop(0, groups // 2, lambda g, _: gram(g), None)
    dft(0)
    lax.fori_loop(groups // 2, groups, lambda g, _: gram(g), None)
    quads = gbuf.shape[1]
    each = modes_k // quads
    for m in range(quads):
        stacked = jnp.concatenate(
            [gs[pl.ds(m * each + r, freqs, stride=modes_k), :] for r in range(each)], axis=0
        )
        gbuf[me_s, m] = stacked.T[: 2 * modes_k]
    for d in range(1, ns):
        copy_g(d).start()
    for b in range(1, blocks):
        dft(b)
    for b in range(blocks):
        inner(b)

    for d in range(1, ns):
        copy_g(d).wait_recv()
    grams = gbuf[0]
    for s in range(1, ns):
        grams = grams + gbuf[s]
    gkj = []
    for j in range(modes_k):
        part = grams[j // each]
        if j % each:
            part = pltpu.roll(part, LANES - (j % each) * freqs, 1)
        gkj.append((part[:modes_k, :freqs], -part[modes_k:, :freqs]))
    diag = jnp.concatenate([gkj[k][0][k : k + 1] for k in range(modes_k)], axis=0)

    def apply_gram(x):
        out = None
        for j in range(modes_k):
            term = mul((x[0][j : j + 1], x[1][j : j + 1]), gkj[j])
            out = term if out is None else add(out, term)
        return out

    def reduced(b):
        for d in range(1, ns):
            copy_p(b, d).wait_recv()
        value = pbuf[b, 0]
        for s in range(1, ns):
            value = value + pbuf[b, s]
        head, tail = value[:modes_k], value[modes_k:]
        proj = head[:, :freqs], pltpu.roll(head, LANES - freqs, 1)[:, :freqs]
        cross = (
            pltpu.roll(tail, LANES - freqs, 1)[:1, :freqs],
            pltpu.roll(tail, LANES - 2 * freqs, 1)[:1, :freqs],
        )
        return proj, tail[:1, :freqs], cross

    shrink = 1.0 / math.sqrt(point_count)
    rate = rates[...]
    b1, qq1, _ = reduced(0)
    a1 = scale(shrink, b1)
    alpha = scale(shrink, a1)
    h1 = sub(b1, apply_gram(alpha))
    rr1 = qq1 - total(mul(alpha, conj(b1)))[0] - total(mul(conj(alpha), h1))[0]
    s1 = scale(rate / jnp.sqrt(qq1 / point_count + 1e-6), conj(a1))
    u1 = diag + 2.0 * mul(s1, h1)[0] + (s1[0] * s1[0] + s1[1] * s1[1]) * rr1
    u1 = jnp.maximum(u1, 0.0)
    id1 = 1.0 / jnp.sqrt(u1 / point_count + 1e-6)
    b2, qq2, q12 = reduced(1)
    rho = sub(q12, total(mul(conj(alpha), b2)))
    a2 = scale(id1 * shrink, add(b2, mul(conj(s1), rho)))
    c2 = scale(id1 * shrink, a2)
    e = total(mul(c2, s1))
    phi_r2 = sub(sub(b2, apply_gram(c2)), mul(e, h1))
    r1_r2 = sub(sub(rho, total(mul(c2, conj(h1)))), scale(rr1, e))
    rr2 = (
        qq2
        - total(mul(c2, conj(b2)))[0]
        - mul(e, conj(rho))[0]
        - total(mul(conj(c2), phi_r2))[0]
        - mul(conj(e), r1_r2)[0]
    )
    s2 = scale(rate / jnp.sqrt(qq2 / point_count + 1e-6), conj(a2))
    p1_r2 = scale(id1, add(phi_r2, mul(conj(s1), r1_r2)))
    u2 = id1 * id1 * u1 + 2.0 * mul(s2, p1_r2)[0] + (s2[0] * s2[0] + s2[1] * s2[1]) * rr2
    id2 = 1.0 / jnp.sqrt(jnp.maximum(u2, 0.0) / point_count + 1e-6)
    keep = id1 * id2
    first, second = scale(keep, s1), scale(id2, s2)
    for ri in range(2):
        coef[0, ri] = a1[ri]
        coef[1, ri] = a2[ri]
    wide = jnp.broadcast_to(e[0], (modes_k, freqs)), jnp.broadcast_to(e[1], (modes_k, freqs))
    for n, value in enumerate((keep, *first, *second, *alpha, *c2, *wide)):
        co[pl.ds(n * modes_k, modes_k), pl.ds(0, freqs)] = value

    for b in range(blocks):
        for d in range(1, nq):
            copy1(b, d).wait_send()
            copy2(b, d).wait_send()
        for d in range(1, ns):
            copy_p(b, d).wait_send()
    for d in range(1, ns):
        copy_g(d).wait_send()


def update_kernel(co, spec, modes, out):
    per, _, fields, modes_k, points = modes.shape
    freqs = spec.shape[2] // 2
    g = pl.program_id(0)
    table = pltpu.roll(co[...], lax.rem(LANES - g * per, LANES), 1)

    def column(n, f):
        return table[n * modes_k : (n + 1) * modes_k, f : f + 1]

    for f in range(per):
        keep, s1r, s1i, s2r, s2i, ar, ai, cr, ci, er, ei = (column(n, f) for n in range(11))
        er, ei = er[:1], ei[:1]
        row_r, row_i = pl.ds(g * per + f, 1), pl.ds(freqs + g * per + f, 1)
        for c in range(fields):
            pr, pi = modes[f, 0, c], modes[f, 1, c]
            r1r = spec[0, c, row_r, :] - jnp.sum(ar * pr - ai * pi, axis=0, keepdims=True)
            r1i = spec[0, c, row_i, :] - jnp.sum(ar * pi + ai * pr, axis=0, keepdims=True)
            r2r = spec[1, c, row_r, :] - jnp.sum(cr * pr - ci * pi, axis=0, keepdims=True)
            r2i = spec[1, c, row_i, :] - jnp.sum(cr * pi + ci * pr, axis=0, keepdims=True)
            r2r = r2r - (er * r1r - ei * r1i)
            r2i = r2i - (er * r1i + ei * r1r)
            out[f, 0, c] = keep * pr + (s1r * r1r - s1i * r1i) + (s2r * r2r - s2i * r2i)
            out[f, 1, c] = keep * pi + (s1r * r1i + s1i * r1r) + (s2r * r2i + s2i * r2r)


def per_device(snapshots, mean_field, weights, rates, modes):
    nq, ns = lax.axis_size("freq"), lax.axis_size("space")
    blocks, quarter, fields, points = snapshots.shape
    freqs, _, modes_k = modes.shape[:3]
    length = quarter * nq
    sub_points = points // nq
    point_count = fields * points * ns
    snap = snapshots.transpose(0, 2, 1, 3)
    field = modes.transpose(0, 1, 3, 2, 4)
    per = LANES * 2 // (2 * modes_k)
    groups = freqs // per
    quads = modes_k * freqs // LANES
    vmem = pl.BlockSpec(memory_space=pltpu.VMEM)
    dma = pltpu.SemaphoreType.DMA
    f32 = jnp.float32
    spec, coef, co = pl.pallas_call(
        functools.partial(spectra_kernel, nq, ns, point_count),
        out_shape=(
            jax.ShapeDtypeStruct((blocks, fields, 2 * freqs, points), f32),
            jax.ShapeDtypeStruct((blocks, 2, modes_k, freqs), f32),
            jax.ShapeDtypeStruct((11 * modes_k, LANES), f32),
        ),
        in_specs=[vmem] * 5 + [pl.BlockSpec(memory_space=pl.ANY)],
        out_specs=(vmem, vmem, vmem),
        scratch_shapes=[
            pltpu.VMEM((freqs, 2, fields, modes_k, points), f32),
            pltpu.VMEM((blocks, fields, length, sub_points), f32),
            pltpu.VMEM((blocks, nq, fields, 2 * freqs, sub_points), f32),
            pltpu.VMEM((fields, 2 * freqs, points), f32),
            pltpu.VMEM((freqs * modes_k, LANES), f32),
            pltpu.VMEM((ns, quads, 2 * modes_k, LANES), f32),
            pltpu.VMEM((blocks, ns, modes_k + 8, LANES), f32),
            dma((groups,)),
            dma((blocks,)),
            dma((blocks,)),
            dma((blocks, nq)),
            dma((blocks, nq)),
            dma((blocks, nq)),
            dma((blocks, nq)),
            dma((ns,)),
            dma((ns,)),
            dma((blocks, ns)),
            dma((blocks, ns)),
        ],
        compiler_params=pltpu.CompilerParams(collective_id=0, has_side_effects=True),
        name="spectra",
    )(
        snap, mean_field, weights, rates.reshape(1, freqs),
        jnp.asarray(spectral_table(length, nq)), field,
    )
    step = 4
    block = (step, 2, fields, modes_k, points)
    updated = pl.pallas_call(
        update_kernel,
        grid=(freqs // step,),
        out_shape=jax.ShapeDtypeStruct(field.shape, f32),
        in_specs=[vmem, vmem, pl.BlockSpec(block, lambda g: (g, 0, 0, 0, 0))],
        out_specs=pl.BlockSpec(block, lambda g: (g, 0, 0, 0, 0)),
        compiler_params=pltpu.CompilerParams(dimension_semantics=("arbitrary",)),
        name="update",
    )(co, spec, field)
    return updated.transpose(0, 1, 3, 2, 4), coef.transpose(0, 3, 1, 2)


def solution(mesh):
    return jax.shard_map(
        per_device,
        mesh=mesh,
        in_specs=(
            P(None, "freq", None, "space"),
            P(None, "space"),
            P(None, "space"),
            P("freq"),
            P("freq", None, None, None, "space"),
        ),
        out_specs=(P("freq", None, None, None, "space"), P(None, "freq", None, None)),
        check_vma=False,
    )
```

```python
import functools
import math

import jax
import jax.numpy as jnp
import numpy as np
from jax import lax
from jax.experimental import pallas as pl
from jax.experimental.pallas import tpu as pltpu
from jax.sharding import PartitionSpec as P

HIGHEST = lax.Precision.HIGHEST
LANES = 128


def spectral_table(length, parts):
    freqs = np.arange(length // 2)
    times = np.arange(length)
    angle = 2.0 * np.pi / length * (freqs[:, None] * times[None, :] % length)
    row = (0.5 - 0.5 * np.cos(2.0 * np.pi / length * times)) / math.sqrt(3.0 * length / 8.0)
    table = np.stack((np.cos(angle) * row, -np.sin(angle) * row))
    table = table.reshape(2, parts, -1, length).transpose(1, 0, 2, 3)
    return table.reshape(length, length).astype(np.float32)


def fold(value):
    total = value[:, :LANES]
    for start in range(LANES, value.shape[1], LANES):
        total = total + value[:, start : start + LANES]
    return total


def split_dot(x, y, axis):
    dims = (((1,), (axis,)), ((), ()))
    xh, yh = x.astype(jnp.bfloat16), y.astype(jnp.bfloat16)
    xl = (x - xh.astype(jnp.float32)).astype(jnp.bfloat16)
    yl = (y - yh.astype(jnp.float32)).astype(jnp.bfloat16)
    dot = functools.partial(lax.dot_general, dimension_numbers=dims, preferred_element_type=jnp.float32)
    return dot(xh, yh) + (dot(xh, yl) + dot(xl, yh))


def mul(x, y):
    return x[0] * y[0] - x[1] * y[1], x[0] * y[1] + x[1] * y[0]


def sub(x, y):
    return x[0] - y[0], x[1] - y[1]


def add(x, y):
    return x[0] + y[0], x[1] + y[1]


def conj(x):
    return x[0], -x[1]


def scale(s, x):
    return s * x[0], s * x[1]


def total(x):
    return jnp.sum(x[0], axis=0, keepdims=True), jnp.sum(x[1], axis=0, keepdims=True)


def spectra_kernel(
    nq, ns, point_count,
    snap, mean, weights, rates, table, modes_hbm,
    spec, coef, co,
    phi, recv, whole, wq, gs, gsend, grecv, gbuf, pbuf,
    phi_sem, own1_sem, own2_sem, send1, recv1, send2, recv2, send_r, recv_r, send_g, recv_g, send_p, recv_p,
):
    blocks, fields, quarter, points = snap.shape
    freqs, _, _, modes_k, _ = phi.shape
    sub_points = points // nq
    groups = phi_sem.shape[0]
    per = freqs // groups
    me_q = lax.axis_index("freq")
    me_s = lax.axis_index("space")

    for g in range(groups):
        pltpu.make_async_copy(
            modes_hbm.at[pl.ds(g * per, per)], phi.at[pl.ds(g * per, per)], phi_sem.at[g]
        ).start()

    barrier = pltpu.get_barrier_semaphore()
    for d in range(1, nq):
        pl.semaphore_signal(
            barrier, inc=1, device_id={"freq": lax.rem(me_q + d, nq)},
            device_id_type=pl.DeviceIdType.MESH,
        )
    for d in range(1, ns):
        pl.semaphore_signal(
            barrier, inc=1, device_id={"space": lax.rem(me_s + d, ns)},
            device_id_type=pl.DeviceIdType.MESH,
        )
    pl.semaphore_wait(barrier, nq + ns - 2)

    def lanes_of(q):
        return pl.ds(pl.multiple_of(q * sub_points, LANES), sub_points)

    def times_of(q):
        return pl.ds(pl.multiple_of(q * quarter, 8), quarter)

    def copy1(b, d):
        to = lax.rem(me_q + d, nq)
        return pltpu.make_async_remote_copy(
            src_ref=snap.at[b, :, :, lanes_of(to)],
            dst_ref=recv.at[b, :, times_of(me_q), :],
            send_sem=send1.at[b, d], recv_sem=recv1.at[b, d],
            device_id={"freq": to}, device_id_type=pl.DeviceIdType.MESH,
        )

    def own1(b):
        return pltpu.make_async_copy(
            snap.at[b, :, :, lanes_of(me_q)], recv.at[b, :, times_of(me_q), :], own1_sem.at[b]
        )

    def copy2(b, d):
        to = lax.rem(me_q + d, nq)
        return pltpu.make_async_remote_copy(
            src_ref=whole.at[b, to],
            dst_ref=spec.at[b, :, :, lanes_of(me_q)],
            send_sem=send2.at[b, d], recv_sem=recv2.at[b, d],
            device_id={"freq": to}, device_id_type=pl.DeviceIdType.MESH,
        )

    def own2(b):
        return pltpu.make_async_copy(
            whole.at[b, me_q], spec.at[b, :, :, lanes_of(me_q)], own2_sem.at[b]
        )

    def copy_r(d):
        to = lax.rem(me_s + d, ns)
        return pltpu.make_async_remote_copy(
            src_ref=gsend.at[to], dst_ref=grecv.at[me_s],
            send_sem=send_r.at[d], recv_sem=recv_r.at[d],
            device_id={"space": to}, device_id_type=pl.DeviceIdType.MESH,
        )

    def copy_g(d):
        return pltpu.make_async_remote_copy(
            src_ref=gbuf.at[me_s], dst_ref=gbuf.at[me_s],
            send_sem=send_g.at[d], recv_sem=recv_g.at[d],
            device_id={"space": lax.rem(me_s + d, ns)}, device_id_type=pl.DeviceIdType.MESH,
        )

    def copy_p(b, d):
        return pltpu.make_async_remote_copy(
            src_ref=pbuf.at[b, me_s], dst_ref=pbuf.at[b, me_s],
            send_sem=send_p.at[b, d], recv_sem=recv_p.at[b, d],
            device_id={"space": lax.rem(me_s + d, ns)}, device_id_type=pl.DeviceIdType.MESH,
        )

    for b in range(blocks):
        for d in range(1, nq):
            copy1(b, d).start()
        own1(b).start()

    def gram(g):
        pltpu.make_async_copy(
            modes_hbm.at[pl.ds(g * per, per)], phi.at[pl.ds(g * per, per)], phi_sem.at[g]
        ).wait()
        rows = per * 2 * modes_k
        product = jnp.zeros((rows, rows), jnp.float32)
        for c in range(fields):
            left = phi[pl.ds(g * per, per), :, c].reshape(rows, points)
            product = product + split_dot(left, left * weights[c : c + 1, :], 1)
        lane = lax.broadcasted_iota(jnp.int32, (modes_k, LANES), 1)
        for f in range(per):
            start = f * 2 * modes_k
            tile = start // LANES * LANES
            block = product[start : start + 2 * modes_k, tile : tile + LANES]
            if start % LANES:
                block = pltpu.roll(block, LANES - start % LANES, 1)
            moved = pltpu.roll(block, LANES - modes_k, 1)
            real = block[:modes_k] + moved[modes_k:]
            imag = moved[:modes_k] - block[modes_k:]
            joined = jnp.where(lane < modes_k, real, pltpu.roll(imag, modes_k, 1))
            gs[pl.ds((g * per + f) * modes_k, modes_k), :] = joined

    def dft(b):
        own1(b).wait()
        for d in range(1, nq):
            copy1(b, d).wait_recv()
        for c in range(fields):
            centered = recv[b, c] - mean[c : c + 1, lanes_of(me_q)]
            rows = split_dot(table[...], centered, 0)
            whole[b, :, c] = rows.reshape(nq, 2 * freqs, sub_points)
        for d in range(1, nq):
            copy2(b, d).start()
        own2(b).start()

    def inner(b):
        own2(b).wait()
        for d in range(1, nq):
            copy2(b, d).wait_recv()
        energy = cross_r = cross_i = jnp.zeros((freqs, LANES), jnp.float32)
        for c in range(fields):
            plain = spec[b, c]
            heavy = plain * weights[c : c + 1, :]
            wq[c] = heavy
            real, imag = heavy[:freqs], heavy[freqs:]
            energy = energy + fold(real * plain[:freqs] + imag * plain[freqs:])
            if b:
                old_r, old_i = spec[b - 1, c, :freqs], spec[b - 1, c, freqs:]
                cross_r = cross_r + fold(old_r * real + old_i * imag)
                cross_i = cross_i + fold(old_r * imag - old_i * real)
        stacked = jnp.concatenate(
            [energy, cross_r, cross_i, jnp.zeros((LANES - 3 * freqs, LANES), jnp.float32)], axis=0
        )
        extra = jnp.sum(stacked.T, axis=0, keepdims=True)
        wide = jnp.broadcast_to(extra, (modes_k, LANES))
        lane = lax.broadcasted_iota(jnp.int32, (modes_k, LANES), 1)

        def body(f, result):
            sum_r = jnp.zeros((modes_k, LANES), jnp.float32)
            sum_i = sum_r
            for c in range(fields):
                row_r, row_i = wq[c, pl.ds(f, 1), :], wq[c, pl.ds(freqs + f, 1), :]
                for start in range(0, points, LANES):
                    tile = slice(start, start + LANES)
                    pr, pi = phi[f, 0, c, :, tile], phi[f, 1, c, :, tile]
                    qr, qi = row_r[:, tile], row_i[:, tile]
                    sum_r = sum_r + (pr * qr + pi * qi)
                    sum_i = sum_i + (pr * qi - pi * qr)
            one_r = jnp.sum(sum_r, axis=1, keepdims=True)
            one_i = jnp.sum(sum_i, axis=1, keepdims=True)
            result = jnp.where(lane == f, one_r, result)
            return jnp.where(lane == freqs + f, one_i, result)

        result = lax.fori_loop(
            0, freqs, body, jnp.zeros((modes_k, LANES), jnp.float32), unroll=4
        )
        row = lax.broadcasted_iota(jnp.int32, (modes_k, LANES), 0)
        side = jnp.where(
            row == 0, pltpu.roll(wide, 2 * freqs, 1),
            jnp.where(row == 1, pltpu.roll(wide, freqs, 1), wide),
        )
        pbuf[b, me_s] = jnp.where(lane < 2 * freqs, result, side)
        for d in range(1, ns):
            copy_p(b, d).start()

    lax.fori_loop(0, groups // 2, lambda g, _: gram(g), None)
    dft(0)
    lax.fori_loop(groups // 2, groups, lambda g, _: gram(g), None)
    each = LANES // freqs
    quads = modes_k // each
    piece = gsend.shape[1]
    owners = 2 * modes_k // piece
    for m in range(quads):
        stacked = jnp.concatenate(
            [gs[pl.ds(m * each + r, freqs, stride=modes_k), :] for r in range(each)], axis=0
        )
        turned = stacked.T
        for o in range(owners):
            gsend[m * owners + o] = turned[o * piece : (o + 1) * piece]
    for d in range(1, ns):
        copy_r(d).start()
    grecv[me_s] = gsend[me_s]
    for b in range(1, blocks):
        dft(b)
    for d in range(1, ns):
        copy_r(d).wait_recv()
    own = grecv[0]
    for s in range(1, ns):
        own = own + grecv[s]
    gbuf[me_s] = own
    for d in range(1, ns):
        copy_g(d).start()
    for b in range(blocks):
        inner(b)

    for d in range(1, ns):
        copy_g(d).wait_recv()
    grams = gbuf[...].reshape(quads, 2 * modes_k, LANES)
    gkj = []
    for j in range(modes_k):
        part = grams[j // each]
        if j % each:
            part = pltpu.roll(part, LANES - (j % each) * freqs, 1)
        gkj.append((part[:modes_k, :freqs], -part[modes_k:, :freqs]))
    diag = jnp.concatenate([gkj[k][0][k : k + 1] for k in range(modes_k)], axis=0)

    def apply_gram(x):
        out = None
        for j in range(modes_k):
            term = mul((x[0][j : j + 1], x[1][j : j + 1]), gkj[j])
            out = term if out is None else add(out, term)
        return out

    def reduced(b):
        for d in range(1, ns):
            copy_p(b, d).wait_recv()
        value = pbuf[b, 0]
        for s in range(1, ns):
            value = value + pbuf[b, s]
        side = pltpu.roll(value, LANES - 2 * freqs, 1)[:, :freqs]
        proj = value[:, :freqs], pltpu.roll(value, LANES - freqs, 1)[:, :freqs]
        return proj, side[:1], (side[1:2], side[2:3])

    shrink = 1.0 / math.sqrt(point_count)
    rate = rates[...]
    b1, qq1, _ = reduced(0)
    a1 = scale(shrink, b1)
    alpha = scale(shrink, a1)
    h1 = sub(b1, apply_gram(alpha))
    rr1 = qq1 - total(mul(alpha, conj(b1)))[0] - total(mul(conj(alpha), h1))[0]
    s1 = scale(rate / jnp.sqrt(qq1 / point_count + 1e-6), conj(a1))
    u1 = diag + 2.0 * mul(s1, h1)[0] + (s1[0] * s1[0] + s1[1] * s1[1]) * rr1
    u1 = jnp.maximum(u1, 0.0)
    id1 = 1.0 / jnp.sqrt(u1 / point_count + 1e-6)
    b2, qq2, q12 = reduced(1)
    rho = sub(q12, total(mul(conj(alpha), b2)))
    a2 = scale(id1 * shrink, add(b2, mul(conj(s1), rho)))
    c2 = scale(id1 * shrink, a2)
    e = total(mul(c2, s1))
    phi_r2 = sub(sub(b2, apply_gram(c2)), mul(e, h1))
    r1_r2 = sub(sub(rho, total(mul(c2, conj(h1)))), scale(rr1, e))
    rr2 = (
        qq2
        - total(mul(c2, conj(b2)))[0]
        - mul(e, conj(rho))[0]
        - total(mul(conj(c2), phi_r2))[0]
        - mul(conj(e), r1_r2)[0]
    )
    s2 = scale(rate / jnp.sqrt(qq2 / point_count + 1e-6), conj(a2))
    p1_r2 = scale(id1, add(phi_r2, mul(conj(s1), r1_r2)))
    u2 = id1 * id1 * u1 + 2.0 * mul(s2, p1_r2)[0] + (s2[0] * s2[0] + s2[1] * s2[1]) * rr2
    id2 = 1.0 / jnp.sqrt(jnp.maximum(u2, 0.0) / point_count + 1e-6)
    keep = id1 * id2
    first, second = scale(keep, s1), scale(id2, s2)
    for ri in range(2):
        coef[0, ri] = a1[ri]
        coef[1, ri] = a2[ri]
    wide = jnp.broadcast_to(e[0], (modes_k, freqs)), jnp.broadcast_to(e[1], (modes_k, freqs))
    for n, value in enumerate((keep, *first, *second, *alpha, *c2, *wide)):
        co[pl.ds(n * modes_k, modes_k), pl.ds(0, freqs)] = value

    for b in range(blocks):
        for d in range(1, nq):
            copy1(b, d).wait_send()
            copy2(b, d).wait_send()
        for d in range(1, ns):
            copy_p(b, d).wait_send()
    for d in range(1, ns):
        copy_r(d).wait_send()
        copy_g(d).wait_send()


def update_kernel(co, spec, modes, out):
    per, _, fields, modes_k, points = modes.shape
    freqs = spec.shape[2] // 2
    g = pl.program_id(0)
    table = pltpu.roll(co[...], lax.rem(LANES - g * per, LANES), 1)

    def column(n, f):
        return table[n * modes_k : (n + 1) * modes_k, f : f + 1]

    for f in range(per):
        keep, s1r, s1i, s2r, s2i, ar, ai, cr, ci, er, ei = (
            jnp.broadcast_to(column(n, f), (modes_k, LANES)) for n in range(11)
        )
        er, ei = er[:1], ei[:1]
        row_r, row_i = pl.ds(g * per + f, 1), pl.ds(freqs + g * per + f, 1)
        for c in range(fields):
            q1r, q1i, q2r, q2i = (spec[b, c, row, :] for b in range(2) for row in (row_r, row_i))
            for start in range(0, points, LANES):
                tile = slice(start, start + LANES)
                pr, pi = modes[f, 0, c, :, tile], modes[f, 1, c, :, tile]
                r1r = q1r[:, tile] - jnp.sum(ar * pr - ai * pi, axis=0, keepdims=True)
                r1i = q1i[:, tile] - jnp.sum(ar * pi + ai * pr, axis=0, keepdims=True)
                r2r = q2r[:, tile] - jnp.sum(cr * pr - ci * pi, axis=0, keepdims=True)
                r2i = q2i[:, tile] - jnp.sum(cr * pi + ci * pr, axis=0, keepdims=True)
                r2r = r2r - (er * r1r - ei * r1i)
                r2i = r2i - (er * r1i + ei * r1r)
                real = keep * pr + (s1r * r1r - s1i * r1i) + (s2r * r2r - s2i * r2i)
                imag = keep * pi + (s1r * r1i + s1i * r1r) + (s2r * r2i + s2i * r2r)
                out[f, 0, c, :, tile] = real
                out[f, 1, c, :, tile] = imag


def per_device(snapshots, mean_field, weights, rates, modes):
    nq, ns = lax.axis_size("freq"), lax.axis_size("space")
    blocks, quarter, fields, points = snapshots.shape
    freqs, _, modes_k = modes.shape[:3]
    length = quarter * nq
    sub_points = points // nq
    point_count = fields * points * ns
    snap = snapshots.transpose(0, 2, 1, 3)
    field = modes.transpose(0, 1, 3, 2, 4)
    per = LANES * 2 // (2 * modes_k)
    groups = freqs // per
    piece = 2 * modes_k * modes_k * freqs // LANES // ns
    vmem = pl.BlockSpec(memory_space=pltpu.VMEM)
    dma = pltpu.SemaphoreType.DMA
    f32 = jnp.float32
    spec, coef, co = pl.pallas_call(
        functools.partial(spectra_kernel, nq, ns, point_count),
        out_shape=(
            jax.ShapeDtypeStruct((blocks, fields, 2 * freqs, points), f32),
            jax.ShapeDtypeStruct((blocks, 2, modes_k, freqs), f32),
            jax.ShapeDtypeStruct((11 * modes_k, LANES), f32),
        ),
        in_specs=[vmem] * 5 + [pl.BlockSpec(memory_space=pl.ANY)],
        out_specs=(vmem, vmem, vmem),
        scratch_shapes=[
            pltpu.VMEM((freqs, 2, fields, modes_k, points), f32),
            pltpu.VMEM((blocks, fields, length, sub_points), f32),
            pltpu.VMEM((blocks, nq, fields, 2 * freqs, sub_points), f32),
            pltpu.VMEM((fields, 2 * freqs, points), f32),
            pltpu.VMEM((freqs * modes_k, LANES), f32),
            pltpu.VMEM((ns, piece, LANES), f32),
            pltpu.VMEM((ns, piece, LANES), f32),
            pltpu.VMEM((ns, piece, LANES), f32),
            pltpu.VMEM((blocks, ns, modes_k, LANES), f32),
            dma((groups,)),
            dma((blocks,)),
            dma((blocks,)),
            dma((blocks, nq)),
            dma((blocks, nq)),
            dma((blocks, nq)),
            dma((blocks, nq)),
            dma((ns,)),
            dma((ns,)),
            dma((ns,)),
            dma((ns,)),
            dma((blocks, ns)),
            dma((blocks, ns)),
        ],
        compiler_params=pltpu.CompilerParams(collective_id=0, has_side_effects=True),
        name="spectra",
    )(
        snap, mean_field, weights, rates.reshape(1, freqs),
        jnp.asarray(spectral_table(length, nq)), field,
    )
    step = 8
    block = (step, 2, fields, modes_k, points)
    updated = pl.pallas_call(
        update_kernel,
        grid=(freqs // step,),
        out_shape=jax.ShapeDtypeStruct(field.shape, f32),
        in_specs=[vmem, vmem, pl.BlockSpec(block, lambda g: (g, 0, 0, 0, 0))],
        out_specs=pl.BlockSpec(block, lambda g: (g, 0, 0, 0, 0)),
        compiler_params=pltpu.CompilerParams(dimension_semantics=("arbitrary",)),
        name="update",
    )(co, spec, field)
    return updated.transpose(0, 1, 3, 2, 4), coef.transpose(0, 3, 1, 2)


def solution(mesh):
    return jax.shard_map(
        per_device,
        mesh=mesh,
        in_specs=(
            P(None, "freq", None, "space"),
            P(None, "space"),
            P(None, "space"),
            P("freq"),
            P("freq", None, None, None, "space"),
        ),
        out_specs=(P("freq", None, None, None, "space"), P(None, "freq", None, None)),
        check_vma=False,
    )
```
